32 devices in a mesh: psg: 8 (over z, x), head: 4 (over y, core).
Axes of the slice: x: 2, y: 2, z: 4, core: 2. Of those that a mesh axis runs over, the one named last changes fastest.
Arguments:
- queries: bfloat16 [64, 2048], P('psg', 'head'), may hold values from -16 to 16
- passage_keys: bfloat16 [16, 256, 2048], P('psg', None, 'head'), may hold values from -6 to 6
- passage_values: bfloat16 [16, 256, 2048], P('psg', None, 'head'), may hold values from -6 to 6
- shelf_ids: int32 [64, 4], P('psg'), may hold values from 0 to 7, all different within a row; in each aligned block of 8 rows (0 to 7, 8 to 15, ...) at most 8 rows name the same one
- live_mask: int32 [64, 8], P('psg'), may hold values 0 or 1
- w_out: bfloat16 [2048, 2048], P('head'), may hold values from -0.75 to 0.75
Outputs:
- out: bfloat16 [64, 2048], P('psg', 'head')
The draws below stay inside these ranges and needn't reach their ends.
Inputs may be any that keep to these rules, and one draw needn't show every extreme that they name: `shelf_ids`: each row names 4 different shelves. Among the rows of one device, no shelf is named by more than 8 rows, and in some devices one shelf is named by exactly 8 rows.
All inputs are finite; a program needn't handle non-finite values. No bound on the sum of `live_mask` on one device may be relied on, other than what follows from the above.
Results may differ from the reference program's by a relative error of at most 0.0085.
Values may be sent and summed in bfloat16 or wider, within the bound.
A program may use at most 64 MiB of HBM per device.

```python
import math
import jax
import jax.numpy as jnp
import numpy as np
from jax import lax

D = 2048
H = 32
DK = 64
LEN = 256
PSG_DEV = 2
REQ_DEV = 8
SHELVES = 4
MOST = 8
HD = 2048
PASSAGES = 16
REQUESTS = 64
ENTRIES = 8
N_PSG = 8


def draw_passage_keys(key, part):
    drawn = jnp.clip(jax.random.normal(jax.random.fold_in(key, 1), (PASSAGES, LEN, HD), jnp.float32), -5.0, 5.0)
    return drawn.astype(jnp.bfloat16)


def draw_queries(key, part):
    drawn = jnp.clip(jax.random.normal(jax.random.fold_in(key, 3), (REQUESTS, HD), jnp.float32), -5.0, 5.0) * 0.3
    return drawn.astype(jnp.bfloat16)


def place_ends(entries, key, low, top_value):
    longest = entries.shape.index(max(entries.shape))
    spots = []
    for shift in (0, 1):
        where = [jax.random.randint(jax.random.fold_in(key, axis), (), 0, length) for axis, length in enumerate(entries.shape)]
        where[longest] = (where[longest] + shift) % entries.shape[longest]
        spots.append(tuple(where))
    return entries.at[spots[0]].set(low).at[spots[1]].set(top_value)


def level_of(own_key, extent, cuts, smallest, largest):
    factor_of, own = 1.0, jax.random.fold_in(own_key, 6)
    for dim, shards_of in cuts:
        heights = jnp.exp(jax.random.uniform(jax.random.fold_in(own, dim), (shards_of,), jnp.float32, smallest / len(cuts), largest / len(cuts)))
        factor_of = factor_of * jnp.repeat(heights, extent[dim] // shards_of).reshape([-1 if axis == dim else 1 for axis in range(len(extent))])
    return factor_of


def assign_block(stream_key, own, number, rows, amount, top, limit, lean):
    order = jax.random.permutation(stream_key, amount)
    crowded, ordinary = shares(amount, rows * top, limit, lean, True), shares(amount, rows * top, limit, lean, False)
    places = jnp.arange(amount)

    def named(tallies, offset_by):
        used = int((tallies > 0).sum())
        fixed = max(1, used // 4)
        shifted = fixed + (places - fixed + offset_by * (used - fixed)) % max(1, amount - fixed)
        return jnp.zeros((amount,), jnp.int32).at[order[jnp.where(places < fixed, places, shifted)]].set(jnp.asarray(tallies, jnp.int32))

    tallies = jnp.where(number % 4 == 0, named(crowded, number // 4), named(ordinary, number - number // 4 - 1))
    mixed = jax.random.permutation(jax.random.fold_in(own, 3), amount)
    source_of, sink = mixed[0:amount // 2 * 2:2], mixed[1:amount // 2 * 2:2]
    slack = jnp.minimum(tallies[source_of] - 1, limit - tallies[sink]) // 2
    slack = jnp.where((source_of == order[0]) | (sink == order[0]) | (tallies[sink] == 0), 0, jnp.maximum(slack, 0))
    shifted = jax.random.randint(jax.random.fold_in(own, 4), (amount // 2,), 0, 1 << 20) % (slack + 1)
    tallies = tallies.at[source_of].add(-shifted).at[sink].add(shifted)
    members = jnp.searchsorted(jnp.cumsum(tallies), jnp.arange(rows * top), side="right").astype(jnp.int32)
    listing = members.reshape(top, rows).T
    listing = listing[jax.random.permutation(jax.random.fold_in(own, 1), rows)]
    offset_by = jax.random.randint(jax.random.fold_in(own, 2), (rows, 1), 0, top)
    return jnp.take_along_axis(listing, (jnp.arange(top)[None, :] + offset_by) % top, axis=1)


def shares(amount, total, reach, lean, full):
    loads = [(1 << 20) // math.isqrt(standing ** lean) + 1 for standing in range(1, amount + 1)]
    largest = reach if full else min(reach, max(-(-total // amount), total * loads[0] // sum(loads)))
    least = 1 if total - largest >= amount - 1 else 0
    counts, surplus = [largest] + [least] * (amount - 1), total - largest - least * (amount - 1)
    while surplus > 0:
        free = [i for i in range(1, amount) if counts[i] < largest] or [i for i in range(1, amount) if counts[i] < reach]
        mass, budget = sum([loads[i] for i in free]), surplus
        for i in free:
            more = min(reach - counts[i], max(1, budget * loads[i] // mass), surplus)
            counts[i] = counts[i] + more
            surplus = surplus - more
    return np.array(counts)


def gaussian(own_key, shape, width, most, shards=(), kind=jnp.bfloat16):
    values = jax.random.normal(own_key, shape, jnp.float32) * width
    if len(shards) > 0:
        values = level_of(own_key, shape, shards, -0.22, 0.18) * values
    return jnp.clip(values, min=-most, max=most).astype(kind)


def setup_inputs(seed: int = 0) -> dict:
    keys = jax.random.split(jax.random.key(seed), 7)
    queries = draw_queries(jax.random.fold_in(keys[6], 71), 0)
    passage_keys = draw_passage_keys(jax.random.fold_in(keys[6], 71), 0)
    passage_values = gaussian(keys[2], (PASSAGES, LEN, HD), 1.0, 6.0, ((0, 8), (2, 4)))
    shelf_ids_keys = jax.random.split(jax.random.fold_in(keys[3], 1), REQUESTS // REQ_DEV)
    shelf_ids_turns = jax.random.permutation(jax.random.fold_in(keys[3], 3), REQUESTS // REQ_DEV)
    shelf_ids = jax.vmap(lambda own, number: assign_block(jax.random.fold_in(keys[3], 2), own, number, REQ_DEV, N_PSG, SHELVES, MOST, 1))(shelf_ids_keys, shelf_ids_turns).reshape((REQUESTS, SHELVES))
    live_mask = place_ends((jax.random.randint(keys[4], (REQUESTS, ENTRIES), 0, 4) < 3).astype(jnp.int32), jax.random.fold_in(keys[4], 1), 0, 1)
    w_out = gaussian(keys[5], (HD, D), (HD // 32) ** -0.5, 0.75, ((0, 4),))
    return dict(queries=queries, passage_keys=passage_keys, passage_values=passage_values, shelf_ids=shelf_ids, live_mask=live_mask, w_out=w_out)


far_below = -1e+30

def shelf_partials(query_rows, live_bits, passage_keys, passage_values):
    row_count = query_rows.shape[0]
    heads_here = query_rows.shape[1] // DK
    passages_here = passage_keys.shape[0]
    length = passage_keys.shape[1]
    query_heads = query_rows.astype(jnp.float32).reshape(row_count, heads_here, DK).transpose(1, 0, 2)
    key_heads = passage_keys.astype(jnp.float32).reshape(passages_here * length, heads_here, DK).transpose(1, 0, 2)
    value_heads = passage_values.astype(jnp.float32).reshape(passages_here * length, heads_here, DK).transpose(1, 0, 2)
    key_live = jnp.repeat(live_bits > 0, length, axis=1)

    def one_head(operands):
        query_head, key_head, value_head = operands
        scores = jnp.dot(query_head, key_head.T)
        scores = jnp.where(key_live, scores, far_below)
        peak_score = jnp.max(scores, axis=1)
        exp_scores = jnp.exp(scores - peak_score[:, None])
        exp_total = jnp.sum(exp_scores, axis=1)
        weights = exp_scores.astype(jnp.bfloat16).astype(jnp.float32)
        context = jnp.dot(weights, value_head) / exp_total[:, None]
        return (context, peak_score, exp_total)
    context, peak_score, exp_total = lax.map(one_head, (query_heads, key_heads, value_heads))
    return (context.transpose(1, 0, 2).reshape(row_count, heads_here * DK), peak_score.T, exp_total.T)

def merge_shelves(context, peak_score, exp_total, has_live):
    request_count, shelf_count, heads_here = peak_score.shape
    masked_peak = jnp.where(has_live[:, :, None], peak_score, far_below)
    best_peak = jnp.max(masked_peak, axis=1)
    shelf_share = jnp.where(has_live[:, :, None], exp_total * jnp.exp(masked_peak - best_peak[:, None, :]), 0.0)
    context_heads = context.reshape(request_count, shelf_count, heads_here, DK)
    attended = jnp.sum(shelf_share[:, :, :, None] * context_heads, axis=1) / jnp.sum(shelf_share, axis=1)[:, :, None]
    return attended.reshape(request_count, heads_here * DK).astype(jnp.bfloat16)

def reference(queries, passage_keys, passage_values, shelf_ids, live_mask, w_out):
    first_entry = (jnp.arange(ENTRIES, dtype=jnp.int32) == 0).astype(jnp.int32)
    live_bits = jnp.maximum(live_mask, first_entry[None, :]).reshape(REQUESTS, SHELVES, PSG_DEV)
    owner_ids = jnp.arange(N_PSG, dtype=jnp.int32)
    presence = jnp.sum((shelf_ids[:, :, None] == owner_ids[None, None, :]).astype(jnp.int32), axis=1)
    blocks = presence.reshape(N_PSG, REQ_DEV, N_PSG)
    rank_table = (jnp.cumsum(blocks, axis=1) - blocks).reshape(REQUESTS, N_PSG).astype(jnp.int32)
    slot_index = jnp.take_along_axis(rank_table, shelf_ids, axis=1).astype(jnp.int32)
    source = (jnp.arange(REQUESTS, dtype=jnp.int32) // REQ_DEV)[:, None]
    box_index = ((shelf_ids * N_PSG + source) * MOST + slot_index).reshape(-1).astype(jnp.int32)
    row_ids = jnp.broadcast_to(jnp.arange(REQUESTS, dtype=jnp.int32)[:, None], (REQUESTS, SHELVES)).reshape(-1)
    box_rows = N_PSG * MOST
    slot_table = jnp.full((N_PSG * box_rows,), REQUESTS, jnp.int32).at[box_index].set(row_ids)
    live_table = jnp.zeros((N_PSG * box_rows, PSG_DEV), jnp.int32).at[box_index].set(live_bits.reshape(-1, PSG_DEV))
    padded = jnp.concatenate([queries, jnp.zeros((1, HD), jnp.bfloat16)], axis=0)

    def owner_work(owner_index):
        start = (owner_index * box_rows).astype(jnp.int32)
        rows = lax.dynamic_slice_in_dim(slot_table, start, box_rows)
        owner_live = lax.dynamic_slice_in_dim(live_table, start, box_rows, 0)
        first_passage = (owner_index * PSG_DEV).astype(jnp.int32)
        owner_keys = lax.dynamic_slice_in_dim(passage_keys, first_passage, PSG_DEV, 0)
        owner_values = lax.dynamic_slice_in_dim(passage_values, first_passage, PSG_DEV, 0)
        return shelf_partials(padded[rows], owner_live, owner_keys, owner_values)
    context, peak_score, exp_total = lax.map(owner_work, owner_ids)
    context = context.reshape(N_PSG * box_rows, HD)[box_index].reshape(REQUESTS, SHELVES, HD)
    peak_score = peak_score.reshape(N_PSG * box_rows, H)[box_index].reshape(REQUESTS, SHELVES, H)
    exp_total = exp_total.reshape(N_PSG * box_rows, H)[box_index].reshape(REQUESTS, SHELVES, H)
    has_live = jnp.max(live_bits, axis=2) > 0
    attended = merge_shelves(context, peak_score, exp_total, has_live)
    return jnp.dot(attended.astype(jnp.float32), w_out.astype(jnp.float32), preferred_element_type=jnp.float32).astype(jnp.bfloat16)
```

```python
import functools

import jax
import jax.numpy as jnp
from jax import lax
from jax.experimental import pallas as pl
from jax.experimental.pallas import tpu as pltpu
from jax.sharding import PartitionSpec as P

DK = 64
far_below = -1e30
LANES = 128
MESH = pl.DeviceIdType.MESH


def each(low, high, body):
    if high - low <= 8:
        for step in range(low, high):
            body(step)
    else:

        @pl.loop(low, high)
        def _(step):
            body(step)


def kernel(
    dims,
    q_hbm,
    k_hbm,
    v_hbm,
    ids_hbm,
    live_hbm,
    w_hbm,
    out_ref,
    k_v,
    v_v,
    w_v,
    ids_v,
    live_v,
    box,
    part,
    stat,
    got_part,
    got_stat,
    rs_out,
    rs_in,
    local_sem,
    q_send,
    q_recv,
    p_send,
    p_recv,
    s_send,
    s_recv,
    r_send,
    r_recv,
):
    owners, groups, rows, width, shelves, passages, length, flag_lanes, group = dims
    me = lax.axis_index("psg")
    my_head = lax.axis_index("head")
    heads = width // DK
    quad = min(256, width)
    quad_heads = quad // DK
    out_cols = w_v.shape[1] // groups

    barrier = pltpu.get_barrier_semaphore()

    def greet_psg(step):
        pl.semaphore_signal(
            barrier, inc=1, device_id={"psg": lax.rem(me + step, owners)}, device_id_type=MESH
        )

    def greet_head(step):
        pl.semaphore_signal(
            barrier,
            inc=1,
            device_id={"head": lax.rem(my_head + step, groups)},
            device_id_type=MESH,
        )

    each(1, owners, greet_psg)
    each(1, groups, greet_head)

    ids_copy = pltpu.make_async_copy(ids_hbm, ids_v, local_sem.at[0])
    live_copy = pltpu.make_async_copy(live_hbm, live_v, local_sem.at[1])
    q_copy = pltpu.make_async_copy(q_hbm, box.at[me, :, pl.ds(0, width)], local_sem.at[2])
    k_copy = pltpu.make_async_copy(k_hbm, k_v, local_sem.at[3])
    v_copy = pltpu.make_async_copy(v_hbm, v_v, local_sem.at[4])
    w_copy = pltpu.make_async_copy(w_hbm, w_v, local_sem.at[5])
    for copy in (ids_copy, live_copy, q_copy, k_copy, v_copy, w_copy):
        copy.start()
    ids_copy.wait()
    live_copy.wait()
    ids = ids_v[...]
    live = live_v[...]
    lane = lax.broadcasted_iota(jnp.int32, (rows, flag_lanes), 1)
    flags = jnp.zeros((rows, flag_lanes), jnp.int32)
    for shelf in range(shelves):
        for p in range(passages):
            entry = shelf * passages + p
            bit = jnp.int32(1) if entry == 0 else live[:, entry : entry + 1]
            flags = jnp.where(lane == ids[:, shelf : shelf + 1] * passages + p, bit, flags)
    q_copy.wait()
    box[me, :, pl.ds(width, flag_lanes)] = flags.astype(jnp.float32).astype(jnp.bfloat16)

    pl.semaphore_wait(barrier, owners + groups - 2)

    def query_copy(peer, source):
        return pltpu.make_async_remote_copy(
            src_ref=box.at[source],
            dst_ref=box.at[source],
            send_sem=q_send.at[peer],
            recv_sem=q_recv.at[source],
            device_id={"psg": peer},
            device_id_type=MESH,
        )

    def part_copy(peer, source):
        return pltpu.make_async_remote_copy(
            src_ref=part.at[peer],
            dst_ref=got_part.at[source],
            send_sem=p_send.at[peer],
            recv_sem=p_recv.at[source],
            device_id={"psg": peer},
            device_id_type=MESH,
        )

    def stat_copy(peer, source):
        return pltpu.make_async_remote_copy(
            src_ref=stat.at[peer],
            dst_ref=got_stat.at[source],
            send_sem=s_send.at[peer],
            recv_sem=s_recv.at[source],
            device_id={"psg": peer},
            device_id_type=MESH,
        )

    def other(step):
        return lax.rem(me + step, owners)

    each(1, owners, lambda step: query_copy(other(step), me).start())
    k_copy.wait()
    v_copy.wait()
    each(1, owners, lambda step: query_copy(me, other(step)).wait_recv())

    block_rows = group * rows
    quad_head = lax.broadcasted_iota(jnp.int32, (block_rows, quad), 1) // DK
    flag_lane = lax.broadcasted_iota(jnp.int32, (block_rows, flag_lanes), 1)
    stat_lane = lax.broadcasted_iota(jnp.int32, (block_rows, LANES), 1)

    def attend(turn):
        first = turn * group
        boxes = box[pl.ds(first, group)].astype(jnp.float32).reshape(block_rows, width + flag_lanes)
        flag = boxes[:, width:]
        bias = []
        for p in range(passages):
            own = jnp.where(flag_lane == me * passages + p, flag, 0.0)
            column = (jnp.sum(own, axis=1, keepdims=True) - 1.0) * -far_below
            bias.append(jnp.concatenate([column] * quad_heads, axis=0))
        stats = jnp.zeros((block_rows, LANES), jnp.float32)
        for g in range(width // quad):
            q = boxes[:, g * quad : (g + 1) * quad]
            spread = jnp.concatenate(
                [jnp.where(quad_head == i, q, 0.0) for i in range(quad_heads)], axis=0
            ).astype(jnp.bfloat16)
            scores = [
                lax.dot_general(
                    spread,
                    k_v[p, :, g * quad : (g + 1) * quad],
                    (((1,), (1,)), ((), ())),
                    preferred_element_type=jnp.float32,
                )
                + bias[p]
                for p in range(passages)
            ]
            peak = functools.reduce(jnp.maximum, scores).max(axis=1, keepdims=True)
            exps = [jnp.exp(s - peak) for s in scores]
            total = functools.reduce(jnp.add, exps).sum(axis=1, keepdims=True)
            mixed = functools.reduce(
                jnp.add,
                [
                    jnp.dot(
                        exps[p].astype(jnp.bfloat16),
                        v_v[p, :, g * quad : (g + 1) * quad],
                        preferred_element_type=jnp.float32,
                    )
                    for p in range(passages)
                ],
            )
            kept = jnp.zeros((block_rows, quad), jnp.float32)
            for i in range(quad_heads):
                span = slice(i * block_rows, (i + 1) * block_rows)
                kept = jnp.where(quad_head == i, mixed[span], kept)
                h = g * quad_heads + i
                stats = jnp.where(stat_lane == h, peak[span], stats)
                stats = jnp.where(stat_lane == heads + h, total[span], stats)
            part[pl.ds(first, group), :, g * quad : (g + 1) * quad] = kept.reshape(
                group, rows, quad
            ).astype(jnp.bfloat16)
        stat[pl.ds(first, group)] = stats.reshape(group, rows, LANES)

    each(0, owners // group, attend)

    def send_back(step):
        part_copy(other(step), me).start()
        stat_copy(other(step), me).start()

    each(1, owners, send_back)
    got_part[me] = part[me]
    got_stat[me] = stat[me]

    def take_back(step):
        stat_copy(me, other(step)).wait_recv()
        part_copy(me, other(step)).wait_recv()

    each(1, owners, take_back)

    every = got_stat[...]
    peaks = every[:, :, :heads]
    totals = every[:, :, heads : 2 * heads]
    scale = jnp.exp(peaks - jnp.max(peaks, axis=0, keepdims=True))
    inverse = 1.0 / jnp.sum(scale * totals, axis=0, keepdims=True)
    share = scale * inverse

    lane_head = lax.broadcasted_iota(jnp.int32, (rows, width), 1) // DK
    attended = jnp.zeros((rows, width), jnp.float32)
    for o in range(owners):
        spread_share = jnp.zeros((rows, width), jnp.float32)
        for h in range(heads):
            spread_share = jnp.where(lane_head == h, share[o, :, h : h + 1], spread_share)
        attended = attended + spread_share * got_part[o].astype(jnp.float32)
    attended = attended.astype(jnp.bfloat16)

    w_copy.wait()

    def project(column):
        cols = pl.ds(pl.multiple_of(column * out_cols, LANES), out_cols)
        return jnp.dot(attended, w_v[:, cols], preferred_element_type=jnp.float32)

    def share_copy(peer, source):
        return pltpu.make_async_remote_copy(
            src_ref=rs_out.at[peer],
            dst_ref=rs_in.at[source],
            send_sem=r_send.at[peer],
            recv_sem=r_recv.at[source],
            device_id={"head": peer},
            device_id_type=MESH,
        )

    for step in range(1, groups):
        peer = lax.rem(my_head + step, groups)
        rs_out[peer] = project(peer).astype(jnp.bfloat16)
        share_copy(peer, my_head).start()
    result = project(my_head)
    for step in range(1, groups):
        source = lax.rem(my_head + step, groups)
        share_copy(my_head, source).wait_recv()
        result = result + rs_in[source].astype(jnp.float32)
    out_ref[...] = result.astype(jnp.bfloat16)

    def drain(step):
        peer = other(step)
        query_copy(peer, me).wait_send()
        part_copy(peer, me).wait_send()
        stat_copy(peer, me).wait_send()

    each(1, owners, drain)
    for step in range(1, groups):
        share_copy(lax.rem(my_head + step, groups), my_head).wait_send()


def per_device(queries, passage_keys, passage_values, shelf_ids, live_mask, w_out):
    owners = lax.axis_size("psg")
    groups = lax.axis_size("head")
    rows, width = queries.shape
    passages, length, _ = passage_keys.shape
    shelves = shelf_ids.shape[1]
    flag_lanes = -(-owners * passages // LANES) * LANES
    group = min(8, owners)
    out_cols = w_out.shape[1] // groups
    dims = (owners, groups, rows, width, shelves, passages, length, flag_lanes, group)
    dma = pltpu.SemaphoreType.DMA
    return pl.pallas_call(
        functools.partial(kernel, dims),
        out_shape=jax.ShapeDtypeStruct((rows, out_cols), jnp.bfloat16),
        in_specs=[pl.BlockSpec(memory_space=pl.ANY)] * 6,
        out_specs=pl.BlockSpec(memory_space=pltpu.VMEM),
        scratch_shapes=[
            pltpu.VMEM(passage_keys.shape, jnp.bfloat16),
            pltpu.VMEM(passage_values.shape, jnp.bfloat16),
            pltpu.VMEM(w_out.shape, jnp.bfloat16),
            pltpu.VMEM(shelf_ids.shape, jnp.int32),
            pltpu.VMEM(live_mask.shape, jnp.int32),
            pltpu.VMEM((owners, rows, width + flag_lanes), jnp.bfloat16),
            pltpu.VMEM((owners, rows, width), jnp.bfloat16),
            pltpu.VMEM((owners, rows, LANES), jnp.float32),
            pltpu.VMEM((owners, rows, width), jnp.bfloat16),
            pltpu.VMEM((owners, rows, LANES), jnp.float32),
            pltpu.VMEM((groups, rows, out_cols), jnp.bfloat16),
            pltpu.VMEM((groups, rows, out_cols), jnp.bfloat16),
            dma((6,)),
            dma((owners,)),
            dma((owners,)),
            dma((owners,)),
            dma((owners,)),
            dma((owners,)),
            dma((owners,)),
            dma((groups,)),
            dma((groups,)),
        ],
        compiler_params=pltpu.CompilerParams(collective_id=0, has_side_effects=True),
    )(queries, passage_keys, passage_values, shelf_ids, live_mask, w_out)


def solution(mesh):
    in_specs = (
        P("psg", "head"),
        P("psg", None, "head"),
        P("psg", None, "head"),
        P("psg", None),
        P("psg", None),
        P("head", None),
    )
    out_specs = P("psg", "head")
    return jax.shard_map(
        per_device, mesh=mesh, in_specs=in_specs, out_specs=out_specs, check_vma=False
    )
```

```python
import functools

import jax
import jax.numpy as jnp
from jax import lax
from jax.experimental import pallas as pl
from jax.experimental.pallas import tpu as pltpu
from jax.sharding import PartitionSpec as P

DK = 64
far_below = -(2.0**100)
LANES = 128
MESH = pl.DeviceIdType.MESH


def each(low, high, body):
    if high - low <= 8:
        for step in range(low, high):
            body(step)
    else:

        @pl.loop(low, high)
        def _(step):
            body(step)


def flip(index, mask):
    bit = 1
    while bit <= mask:
        if mask & bit:
            index = index + bit * (1 - 2 * (index // bit % 2))
        bit *= 2
    return index


def kernel(
    dims,
    q_hbm,
    k_hbm,
    v_hbm,
    ids_hbm,
    live_hbm,
    w_hbm,
    out_ref,
    k_v,
    v_v,
    w_v,
    ids_v,
    live_v,
    box,
    part,
    got_part,
    rs_out,
    rs_in,
    local_sem,
    q_send,
    q_recv,
    p_send,
    p_recv,
    r_send,
    r_recv,
):
    owners, groups, rows, width, shelves, passages, length, flag_lanes, group = dims
    me = lax.axis_index("psg")
    my_head = lax.axis_index("head")
    heads = width // DK
    quad = min(256, width)
    quad_heads = quad // DK
    out_cols = w_v.shape[1] // groups

    barrier = pltpu.get_barrier_semaphore()

    def greet_psg(step):
        pl.semaphore_signal(
            barrier, inc=1, device_id={"psg": lax.rem(me + step, owners)}, device_id_type=MESH
        )

    def greet_head(step):
        pl.semaphore_signal(
            barrier,
            inc=1,
            device_id={"head": lax.rem(my_head + step, groups)},
            device_id_type=MESH,
        )

    each(1, owners, greet_psg)
    each(1, groups, greet_head)

    ids_copy = pltpu.make_async_copy(ids_hbm, ids_v, local_sem.at[0])
    live_copy = pltpu.make_async_copy(live_hbm, live_v, local_sem.at[1])
    q_copy = pltpu.make_async_copy(q_hbm, box.at[me, :, pl.ds(0, width)], local_sem.at[2])
    k_copy = pltpu.make_async_copy(k_hbm, k_v, local_sem.at[3])
    v_copy = pltpu.make_async_copy(v_hbm, v_v, local_sem.at[4])
    w_copy = pltpu.make_async_copy(w_hbm, w_v, local_sem.at[5])
    for copy in (ids_copy, live_copy, q_copy, k_copy, v_copy, w_copy):
        copy.start()
    ids_copy.wait()
    live_copy.wait()
    ids_row = ids_v[...].astype(jnp.float32)
    square = (rows, rows)
    on_diagonal = lax.broadcasted_iota(jnp.int32, square, 0) == lax.broadcasted_iota(
        jnp.int32, square, 1
    )
    ids = [
        jnp.sum(
            jnp.where(on_diagonal, jnp.broadcast_to(ids_row[j : j + 1], square), 0.0),
            axis=1,
            keepdims=True,
        ).astype(jnp.int32)
        for j in range(shelves)
    ]
    live = live_v[...]
    lane = lax.broadcasted_iota(jnp.int32, (rows, flag_lanes), 1)
    flags = jnp.zeros((rows, flag_lanes), jnp.int32)
    assert 3 * heads <= LANES
    for shelf in range(shelves):
        for p in range(passages):
            entry = shelf * passages + p
            bit = jnp.int32(1) if entry == 0 else live[:, entry : entry + 1]
            flags = jnp.where(lane == ids[shelf] * passages + p, bit, flags)
    q_copy.wait()
    box[me, :, pl.ds(width, flag_lanes)] = flags.astype(jnp.float32).astype(jnp.bfloat16)

    pl.semaphore_wait(barrier, owners + groups - 2)

    def query_copy(peer, source):
        return pltpu.make_async_remote_copy(
            src_ref=box.at[source],
            dst_ref=box.at[source],
            send_sem=q_send.at[peer],
            recv_sem=q_recv.at[source],
            device_id={"psg": peer},
            device_id_type=MESH,
        )

    def part_copy(peer, source):
        return pltpu.make_async_remote_copy(
            src_ref=part.at[peer],
            dst_ref=got_part.at[source],
            send_sem=p_send.at[peer],
            recv_sem=p_recv.at[source],
            device_id={"psg": peer},
            device_id_type=MESH,
        )

    turns = owners // group
    my_turn = me // group
    my_place = me % group

    def peer_of(turn, place):
        return (my_turn + turn) % turns * group + (my_place + place) % group

    def each_peer(turn, body):
        each(0, group, lambda place: body(peer_of(turn, place)))

    def each_near(body):
        each(1, group, lambda place: body(peer_of(0, place)))

    def send_query(peer):
        query_copy(peer, me).start()

    def take_query(source):
        query_copy(me, source).wait_recv()

    def send_part(peer):
        part_copy(peer, me).start()

    def take_part(source):
        part_copy(me, source).wait_recv()

    def drain(peer):
        query_copy(peer, me).wait_send()
        part_copy(peer, me).wait_send()

    each(1, turns, lambda turn: each_peer(turn, send_query))
    each_near(send_query)
    k_copy.wait()
    v_copy.wait()

    block_rows = group * rows
    quad_head = lax.broadcasted_iota(jnp.int32, (block_rows, quad), 1) // DK
    flag_lane = lax.broadcasted_iota(jnp.int32, (block_rows, flag_lanes), 1)
    stat_lane = lax.broadcasted_iota(jnp.int32, (block_rows, LANES), 1)

    def attend(turn):
        first = (my_turn + turn) % turns * group
        boxes = box[pl.ds(first, group)].astype(jnp.float32).reshape(block_rows, width + flag_lanes)
        flag = boxes[:, width:]
        bias = []
        for p in range(passages):
            own = jnp.where(flag_lane == me * passages + p, flag, 0.0)
            column = (jnp.sum(own, axis=1, keepdims=True) - 1.0) * -far_below
            bias.append(jnp.concatenate([column] * quad_heads, axis=0))
        stats = jnp.zeros((block_rows, LANES), jnp.float32)
        for g in range(width // quad):
            q = boxes[:, g * quad : (g + 1) * quad]
            spread = jnp.concatenate(
                [jnp.where(quad_head == i, q, 0.0) for i in range(quad_heads)], axis=0
            ).astype(jnp.bfloat16)
            scores = [
                lax.dot_general(
                    spread,
                    k_v[p, :, g * quad : (g + 1) * quad],
                    (((1,), (1,)), ((), ())),
                    preferred_element_type=jnp.float32,
                )
                + bias[p]
                for p in range(passages)
            ]
            peak = functools.reduce(jnp.maximum, scores).max(axis=1, keepdims=True)
            peak = peak.astype(jnp.bfloat16).astype(jnp.float32)
            exps = [jnp.exp(s - peak) for s in scores]
            total = functools.reduce(jnp.add, exps).sum(axis=1, keepdims=True)
            coarse = total.astype(jnp.bfloat16).astype(jnp.float32)
            mixed = functools.reduce(
                jnp.add,
                [
                    jnp.dot(
                        exps[p].astype(jnp.bfloat16),
                        v_v[p, :, g * quad : (g + 1) * quad],
                        preferred_element_type=jnp.float32,
                    )
                    for p in range(passages)
                ],
            )
            kept = jnp.zeros((block_rows, quad), jnp.float32)
            for i in range(quad_heads):
                span = slice(i * block_rows, (i + 1) * block_rows)
                kept = jnp.where(quad_head == i, mixed[span], kept)
                h = g * quad_heads + i
                stats = jnp.where(stat_lane == h, peak[span], stats)
                stats = jnp.where(stat_lane == heads + h, coarse[span], stats)
                stats = jnp.where(stat_lane == 2 * heads + h, (total - coarse)[span], stats)
            part[pl.ds(first, group), :, g * quad : (g + 1) * quad] = kept.reshape(
                group, rows, quad
            ).astype(jnp.bfloat16)
        part[pl.ds(first, group), :, width:] = stats.reshape(group, rows, LANES).astype(
            jnp.bfloat16
        )

    each_near(take_query)
    attend(0)
    each_near(send_part)
    got_part[me] = part[me]

    def far_turn(turn):
        each_peer(turn, take_query)
        attend(turn)
        each_peer(turn, send_part)

    each(1, turns, far_turn)
    each_near(take_part)
    each(1, turns, lambda turn: each_peer(turn, take_part))

    every = got_part[:, :, width:].astype(jnp.float32)
    peaks = every[:, :, :heads]
    totals = every[:, :, heads : 2 * heads] + every[:, :, 2 * heads : 3 * heads]
    scale = jnp.exp(peaks - jnp.max(peaks, axis=0, keepdims=True))
    inverse = 1.0 / jnp.sum(scale * totals, axis=0, keepdims=True)
    share = scale * inverse

    lane_head = lax.broadcasted_iota(jnp.int32, (rows, width), 1) // DK
    attended = jnp.zeros((rows, width), jnp.float32)
    for o in range(owners):
        spread_share = jnp.zeros((rows, width), jnp.float32)
        for h in range(heads):
            spread_share = jnp.where(lane_head == h, share[o, :, h : h + 1], spread_share)
        attended = attended + spread_share * got_part[o, :, :width].astype(jnp.float32)
    attended = attended.astype(jnp.bfloat16)

    w_copy.wait()

    def project(column):
        cols = pl.ds(pl.multiple_of(column * out_cols, LANES), out_cols)
        return jnp.dot(attended, w_v[:, cols], preferred_element_type=jnp.float32)

    def share_copy(peer, source):
        return pltpu.make_async_remote_copy(
            src_ref=rs_out.at[peer],
            dst_ref=rs_in.at[source],
            send_sem=r_send.at[peer],
            recv_sem=r_recv.at[source],
            device_id={"head": peer},
            device_id_type=MESH,
        )

    if groups & (groups - 1) == 0:
        partners = [flip(my_head, mask) for mask in range(groups - 1, 0, -1)]
    else:
        partners = [lax.rem(my_head + step, groups) for step in range(1, groups)]
    for peer in partners:
        rs_out[peer] = project(peer).astype(jnp.bfloat16)
        share_copy(peer, my_head).start()
    result = project(my_head)
    for peer in reversed(partners):
        share_copy(my_head, peer).wait_recv()
        result = result + rs_in[peer].astype(jnp.float32)
    out_ref[...] = result.astype(jnp.bfloat16)

    each_near(drain)
    each(1, turns, lambda turn: each_peer(turn, drain))
    for peer in partners:
        share_copy(peer, my_head).wait_send()


def per_device(queries, passage_keys, passage_values, shelf_ids, live_mask, w_out):
    owners = lax.axis_size("psg")
    groups = lax.axis_size("head")
    rows, width = queries.shape
    passages, length, _ = passage_keys.shape
    shelves = shelf_ids.shape[1]
    flag_lanes = -(-owners * passages // LANES) * LANES
    group = next(size for size in (8, 4, 2, 1) if owners % size == 0 and size < owners)
    out_cols = w_out.shape[1] // groups
    dims = (owners, groups, rows, width, shelves, passages, length, flag_lanes, group)
    dma = pltpu.SemaphoreType.DMA
    return pl.pallas_call(
        functools.partial(kernel, dims),
        out_shape=pltpu.VMEM((rows, out_cols), jnp.bfloat16),
        in_specs=[pl.BlockSpec(memory_space=pl.ANY)] * 6,
        out_specs=pl.BlockSpec(memory_space=pltpu.VMEM),
        scratch_shapes=[
            pltpu.VMEM(passage_keys.shape, jnp.bfloat16),
            pltpu.VMEM(passage_values.shape, jnp.bfloat16),
            pltpu.VMEM(w_out.shape, jnp.bfloat16),
            pltpu.VMEM((shelves, rows), jnp.int32),
            pltpu.VMEM(live_mask.shape, jnp.int32),
            pltpu.VMEM((owners, rows, width + flag_lanes), jnp.bfloat16),
            pltpu.VMEM((owners, rows, width + LANES), jnp.bfloat16),
            pltpu.VMEM((owners, rows, width + LANES), jnp.bfloat16),
            pltpu.VMEM((groups, rows, out_cols), jnp.bfloat16),
            pltpu.VMEM((groups, rows, out_cols), jnp.bfloat16),
            dma((6,)),
            dma((owners,)),
            dma((owners,)),
            dma((owners,)),
            dma((owners,)),
            dma((groups,)),
            dma((groups,)),
        ],
        compiler_params=pltpu.CompilerParams(collective_id=0, has_side_effects=True),
    )(queries, passage_keys, passage_values, shelf_ids.T, live_mask, w_out)


def solution(mesh):
    in_specs = (
        P("psg", "head"),
        P("psg", None, "head"),
        P("psg", None, "head"),
        P("psg", None),
        P("psg", None),
        P("head", None),
    )
    out_specs = P("psg", "head")
    return jax.shard_map(
        per_device, mesh=mesh, in_specs=in_specs, out_specs=out_specs, check_vma=False
    )
```

```python
import functools

import jax
import jax.numpy as jnp
from jax import lax
from jax.experimental import pallas as pl
from jax.experimental.pallas import tpu as pltpu
from jax.sharding import PartitionSpec as P

DK = 64
far_below = -(2.0**100)
LANES = 128
MESH = pl.DeviceIdType.MESH


def each(low, high, body):
    if high - low <= 8:
        for step in range(low, high):
            body(step)
    else:

        @pl.loop(low, high)
        def _(step):
            body(step)


def flip(index, mask):
    bit = 1
    while bit <= mask:
        if mask & bit:
            index = index + bit * (1 - 2 * (index // bit % 2))
        bit *= 2
    return index


def kernel(
    dims,
    q_hbm,
    k_hbm,
    v_hbm,
    ids_hbm,
    live_hbm,
    w_hbm,
    out_ref,
    k_v,
    v_v,
    w_v,
    ids_v,
    live_v,
    box,
    part,
    got_part,
    rs_out,
    rs_in,
    local_sem,
    q_send,
    q_recv,
    p_send,
    p_recv,
    r_send,
    r_recv,
):
    owners, groups, rows, width, shelves, passages, length, flag_lanes, group = dims
    me = lax.axis_index("psg")
    my_head = lax.axis_index("head")
    heads = width // DK
    quad = min(256, width)
    quad_heads = quad // DK
    out_cols = w_v.shape[1] // groups

    barrier = pltpu.get_barrier_semaphore()

    def greet_psg(step):
        pl.semaphore_signal(
            barrier, inc=1, device_id={"psg": lax.rem(me + step, owners)}, device_id_type=MESH
        )

    def greet_head(step):
        pl.semaphore_signal(
            barrier,
            inc=1,
            device_id={"head": lax.rem(my_head + step, groups)},
            device_id_type=MESH,
        )

    each(1, owners, greet_psg)
    each(1, groups, greet_head)

    ids_copy = pltpu.make_async_copy(ids_hbm, ids_v, local_sem.at[0])
    live_copy = pltpu.make_async_copy(live_hbm, live_v, local_sem.at[1])
    q_copy = pltpu.make_async_copy(q_hbm, box.at[me, :, pl.ds(0, width)], local_sem.at[2])
    k_copy = pltpu.make_async_copy(k_hbm, k_v, local_sem.at[3])
    v_copy = pltpu.make_async_copy(v_hbm, v_v, local_sem.at[4])
    w_copy = pltpu.make_async_copy(w_hbm, w_v, local_sem.at[5])
    for copy in (ids_copy, live_copy, q_copy, k_copy, v_copy, w_copy):
        copy.start()
    ids_copy.wait()
    live_copy.wait()
    ids_row = ids_v[...].astype(jnp.float32)
    square = (rows, rows)
    on_diagonal = lax.broadcasted_iota(jnp.int32, square, 0) == lax.broadcasted_iota(
        jnp.int32, square, 1
    )
    ids = [
        jnp.sum(
            jnp.where(on_diagonal, jnp.broadcast_to(ids_row[j : j + 1], square), 0.0),
            axis=1,
            keepdims=True,
        ).astype(jnp.int32)
        for j in range(shelves)
    ]
    live = live_v[...]
    lane = lax.broadcasted_iota(jnp.int32, (rows, flag_lanes), 1)
    flags = jnp.zeros((rows, flag_lanes), jnp.int32)
    assert 3 * heads <= LANES
    for shelf in range(shelves):
        for p in range(passages):
            entry = shelf * passages + p
            bit = jnp.int32(1) if entry == 0 else live[:, entry : entry + 1]
            flags = jnp.where(lane == ids[shelf] * passages + p, bit, flags)
    q_copy.wait()
    box[me, :, pl.ds(width, flag_lanes)] = flags.astype(jnp.float32).astype(jnp.bfloat16)

    pl.semaphore_wait(barrier, owners + groups - 2)

    def query_copy(peer, source):
        return pltpu.make_async_remote_copy(
            src_ref=box.at[source],
            dst_ref=box.at[source],
            send_sem=q_send.at[peer],
            recv_sem=q_recv.at[source],
            device_id={"psg": peer},
            device_id_type=MESH,
        )

    def part_copy(peer, source):
        return pltpu.make_async_remote_copy(
            src_ref=part.at[peer],
            dst_ref=got_part.at[source],
            send_sem=p_send.at[peer],
            recv_sem=p_recv.at[source],
            device_id={"psg": peer},
            device_id_type=MESH,
        )

    turns = owners // group
    my_turn = me // group
    my_place = me % group

    def block_of(turn):
        if isinstance(turn, int) and turns & (turns - 1) == 0:
            return flip(my_turn, turn)
        return (my_turn + turn) % turns

    def peer_of(turn, place):
        return block_of(turn) * group + (my_place + place) % group

    def each_peer(turn, body):
        each(0, group, lambda place: body(peer_of(turn, place)))

    def each_near(body):
        each(1, group, lambda place: body(peer_of(0, place)))

    def send_query(peer):
        query_copy(peer, me).start()

    def take_query(source):
        query_copy(me, source).wait_recv()

    def send_part(peer):
        part_copy(peer, me).start()

    def take_part(source):
        part_copy(me, source).wait_recv()

    def drain(peer):
        query_copy(peer, me).wait_send()
        part_copy(peer, me).wait_send()

    each(1, turns, lambda turn: each_peer(turns - turn, send_query))
    each_near(send_query)
    k_copy.wait()
    v_copy.wait()

    block_rows = group * rows
    quad_head = lax.broadcasted_iota(jnp.int32, (block_rows, quad), 1) // DK
    flag_lane = lax.broadcasted_iota(jnp.int32, (block_rows, flag_lanes), 1)
    stat_lane = lax.broadcasted_iota(jnp.int32, (block_rows, LANES), 1)

    def attend(turn):
        first = block_of(turn) * group
        boxes = box[pl.ds(first, group)].astype(jnp.float32).reshape(block_rows, width + flag_lanes)
        flag = boxes[:, width:]
        bias = []
        for p in range(passages):
            own = jnp.where(flag_lane == me * passages + p, flag, 0.0)
            column = (jnp.sum(own, axis=1, keepdims=True) - 1.0) * -far_below
            bias.append(jnp.concatenate([column] * quad_heads, axis=0))
        stats = jnp.zeros((block_rows, LANES), jnp.float32)
        for g in range(width // quad):
            q = boxes[:, g * quad : (g + 1) * quad]
            spread = jnp.concatenate(
                [jnp.where(quad_head == i, q, 0.0) for i in range(quad_heads)], axis=0
            ).astype(jnp.bfloat16)
            scores = [
                lax.dot_general(
                    spread,
                    k_v[p, :, g * quad : (g + 1) * quad],
                    (((1,), (1,)), ((), ())),
                    preferred_element_type=jnp.float32,
                )
                + bias[p]
                for p in range(passages)
            ]
            peak = functools.reduce(jnp.maximum, scores).max(axis=1, keepdims=True)
            peak = peak.astype(jnp.bfloat16).astype(jnp.float32)
            exps = [jnp.exp(s - peak) for s in scores]
            total = functools.reduce(jnp.add, exps).sum(axis=1, keepdims=True)
            coarse = total.astype(jnp.bfloat16).astype(jnp.float32)
            mixed = functools.reduce(
                jnp.add,
                [
                    jnp.dot(
                        exps[p].astype(jnp.bfloat16),
                        v_v[p, :, g * quad : (g + 1) * quad],
                        preferred_element_type=jnp.float32,
                    )
                    for p in range(passages)
                ],
            )
            kept = jnp.zeros((block_rows, quad), jnp.float32)
            for i in range(quad_heads):
                span = slice(i * block_rows, (i + 1) * block_rows)
                kept = jnp.where(quad_head == i, mixed[span], kept)
                h = g * quad_heads + i
                stats = jnp.where(stat_lane == h, peak[span], stats)
                stats = jnp.where(stat_lane == heads + h, coarse[span], stats)
                stats = jnp.where(stat_lane == 2 * heads + h, (total - coarse)[span], stats)
            part[pl.ds(first, group), :, g * quad : (g + 1) * quad] = kept.reshape(
                group, rows, quad
            ).astype(jnp.bfloat16)
        part[pl.ds(first, group), :, width:] = stats.reshape(group, rows, LANES).astype(
            jnp.bfloat16
        )

    each_near(take_query)
    attend(0)
    each_near(send_part)
    got_part[me] = part[me]

    def far_turn(turn):
        each_peer(turn, take_query)
        attend(turn)
        each_peer(turn, send_part)

    each(1, turns, far_turn)
    each_near(take_part)
    each(1, turns, lambda turn: each_peer(turn, take_part))

    every = got_part[:, :, width:].astype(jnp.float32)
    peaks = every[:, :, :heads]
    totals = every[:, :, heads : 2 * heads] + every[:, :, 2 * heads : 3 * heads]
    scale = jnp.exp(peaks - jnp.max(peaks, axis=0, keepdims=True))
    inverse = 1.0 / jnp.sum(scale * totals, axis=0, keepdims=True)
    share = scale * inverse

    high_half = lax.broadcasted_iota(jnp.int32, (rows, LANES), 1) // DK
    per_tile = LANES // DK
    columns = [jnp.zeros((rows, LANES), jnp.float32) for _ in range(width // LANES)]
    for o in range(owners):
        for c in range(width // LANES):
            weight = share[o, :, c * per_tile : c * per_tile + 1]
            for i in range(1, per_tile):
                h = c * per_tile + i
                weight = jnp.where(high_half == i, share[o, :, h : h + 1], weight)
            columns[c] = columns[c] + weight * got_part[
                o, :, c * LANES : (c + 1) * LANES
            ].astype(jnp.float32)
    attended = jnp.concatenate(columns, axis=1)
    attended = attended.astype(jnp.bfloat16)

    w_copy.wait()

    def project(column):
        cols = pl.ds(pl.multiple_of(column * out_cols, LANES), out_cols)
        return jnp.dot(attended, w_v[:, cols], preferred_element_type=jnp.float32)

    def share_copy(peer, source):
        return pltpu.make_async_remote_copy(
            src_ref=rs_out.at[peer],
            dst_ref=rs_in.at[source],
            send_sem=r_send.at[peer],
            recv_sem=r_recv.at[source],
            device_id={"head": peer},
            device_id_type=MESH,
        )

    if groups & (groups - 1) == 0:
        partners = [flip(my_head, mask) for mask in range(groups - 1, 0, -1)]
    else:
        partners = [lax.rem(my_head + step, groups) for step in range(1, groups)]
    for peer in partners:
        rs_out[peer] = project(peer).astype(jnp.bfloat16)
        share_copy(peer, my_head).start()
    result = project(my_head)
    for peer in reversed(partners):
        share_copy(my_head, peer).wait_recv()
        result = result + rs_in[peer].astype(jnp.float32)
    out_ref[...] = result.astype(jnp.bfloat16)

    each_near(drain)
    each(1, turns, lambda turn: each_peer(turn, drain))
    for peer in partners:
        share_copy(peer, my_head).wait_send()


def per_device(queries, passage_keys, passage_values, shelf_ids, live_mask, w_out):
    owners = lax.axis_size("psg")
    groups = lax.axis_size("head")
    rows, width = queries.shape
    passages, length, _ = passage_keys.shape
    shelves = shelf_ids.shape[1]
    flag_lanes = -(-owners * passages // LANES) * LANES
    group = next(size for size in (8, 4, 2, 1) if owners % (2 * size) == 0 or size == 1)
    out_cols = w_out.shape[1] // groups
    dims = (owners, groups, rows, width, shelves, passages, length, flag_lanes, group)
    dma = pltpu.SemaphoreType.DMA
    return pl.pallas_call(
        functools.partial(kernel, dims),
        out_shape=pltpu.VMEM((rows, out_cols), jnp.bfloat16),
        in_specs=[pl.BlockSpec(memory_space=pl.ANY)] * 6,
        out_specs=pl.BlockSpec(memory_space=pltpu.VMEM),
        scratch_shapes=[
            pltpu.VMEM(passage_keys.shape, jnp.bfloat16),
            pltpu.VMEM(passage_values.shape, jnp.bfloat16),
            pltpu.VMEM(w_out.shape, jnp.bfloat16),
            pltpu.VMEM((shelves, rows), jnp.int32),
            pltpu.VMEM(live_mask.shape, jnp.int32),
            pltpu.VMEM((owners, rows, width + flag_lanes), jnp.bfloat16),
            pltpu.VMEM((owners, rows, width + LANES), jnp.bfloat16),
            pltpu.VMEM((owners, rows, width + LANES), jnp.bfloat16),
            pltpu.VMEM((groups, rows, out_cols), jnp.bfloat16),
            pltpu.VMEM((groups, rows, out_cols), jnp.bfloat16),
            dma((6,)),
            dma((owners,)),
            dma((owners,)),
            dma((owners,)),
            dma((owners,)),
            dma((groups,)),
            dma((groups,)),
        ],
        compiler_params=pltpu.CompilerParams(collective_id=0, has_side_effects=True),
    )(queries, passage_keys, passage_values, shelf_ids.T, live_mask, w_out)


def solution(mesh):
    in_specs = (
        P("psg", "head"),
        P("psg", None, "head"),
        P("psg", None, "head"),
        P("psg", None),
        P("psg", None),
        P("head", None),
    )
    out_specs = P("psg", "head")
    return jax.shard_map(
        per_device, mesh=mesh, in_specs=in_specs, out_specs=out_specs, check_vma=False
    )
```
